64 devices in a mesh: dp: 4 (over x, y), cp: 16 (over z, core).
Axes of the slice: x: 2, y: 2, z: 8, core: 2. Of those that a mesh axis runs over, the one named last changes fastest.
The devices are a block of a 4x4x8 slice.
Arguments:
- x_seq: bfloat16 [4, 8192, 512], P('dp', 'cp'), parts along dimension 0
- dy_seq: float32 [4, 8192, 512], P('dp', 'cp'), parts along dimension 0
- ln1_gain: float32 [512], replicated
- ln1_bias: float32 [512], replicated
- ln2_gain: float32 [512], replicated
- ln2_bias: float32 [512], replicated
- w_qkv: bfloat16 [512, 8, 3, 64], replicated
- b_qkv: bfloat16 [8, 3, 64], replicated
- w_out: bfloat16 [512, 512], replicated
- b_out: bfloat16 [512], replicated
- w_up: bfloat16 [512, 2048], replicated
- b_up: bfloat16 [2048], replicated
- w_down: bfloat16 [2048, 512], replicated
- b_down: bfloat16 [512], replicated
Outputs:
- output 1: bfloat16 [4, 8192, 512], P('dp', 'cp'), parts along dimension 0
- output 2: float32 [4, 8192, 512], P('dp', 'cp'), parts along dimension 0
- output 3: float32 [2048], P('dp'), parts along dimension 0
- output 4: float32 [2048], P('dp'), parts along dimension 0
- output 5: float32 [2048], P('dp'), parts along dimension 0
- output 6: float32 [2048], P('dp'), parts along dimension 0
- output 7: float32 [2048, 8, 3, 64], P('dp'), parts along dimension 0
- output 8: float32 [32, 3, 64], P('dp'), parts along dimension 0
- output 9: float32 [2048, 512], P('dp'), parts along dimension 0
- output 10: float32 [2048], P('dp'), parts along dimension 0
- output 11: float32 [2048, 2048], P('dp'), parts along dimension 0
- output 12: float32 [8192], P('dp'), parts along dimension 0
- output 13: float32 [8192, 512], P('dp'), parts along dimension 0
- output 14: float32 [2048], P('dp'), parts along dimension 0
There are 4 independent parts. The reference program is written for one: setup_inputs(seed, part) draws one part's arguments, and reference() takes and returns one part's arrays. A program takes and returns all parts, laid end to end along the dimension named above; an argument that names none is the same for every part.
All inputs are finite; a program needn't handle non-finite values.
Results may differ from the reference program's by a relative error of at most 0.0196811.
Values are sent between devices in bfloat16 or wider.
A program may use at most 768 MiB of HBM per device.

```python
import math
import jax
import jax.numpy as jnp
from jax import lax

D = 512
HEADS = 8
HEAD = 64
FF = 2048
BATCH = 1
SEQ = 8192
ROT = HEAD // 4
QBLK = min(SEQ, 128)
EPS = 1e-5
ROPE_BASE = 10000.0
NEG_BIG = -1e30


def setup_inputs(seed: int = 0, part: int = 0) -> dict:
    part_key = jax.random.fold_in(jax.random.key(seed), part)
    act_keys = jax.random.split(part_key, 2)
    weight_keys = jax.random.split(jax.random.key(seed + 1), 12)
    qk_gain = max(math.log(SEQ / 16.0), 1.0) ** 0.25
    col_scale = jnp.array([qk_gain, qk_gain, 1.0], dtype=jnp.float32)[None, None, :, None] * D ** -0.5

    def normal(rand_key, arr_shape):
        return jax.random.normal(rand_key, arr_shape, dtype=jnp.float32)

    return {
        'x_seq': normal(act_keys[0], (BATCH, SEQ, D)).astype(jnp.bfloat16),
        'dy_seq': normal(act_keys[1], (BATCH, SEQ, D)),
        'ln1_gain': 1.0 + 0.3 * normal(weight_keys[0], (D,)),
        'ln1_bias': 0.3 * normal(weight_keys[1], (D,)),
        'ln2_gain': 1.0 + 0.3 * normal(weight_keys[2], (D,)),
        'ln2_bias': 0.3 * normal(weight_keys[3], (D,)),
        'w_qkv': (normal(weight_keys[4], (D, HEADS, 3, HEAD)) * col_scale).astype(jnp.bfloat16),
        'b_qkv': (0.3 * normal(weight_keys[5], (HEADS, 3, HEAD))).astype(jnp.bfloat16),
        'w_out': (2.0 * D ** -0.5 * normal(weight_keys[6], (D, D))).astype(jnp.bfloat16),
        'b_out': (0.3 * normal(weight_keys[7], (D,))).astype(jnp.bfloat16),
        'w_up': (D ** -0.5 * normal(weight_keys[8], (D, FF))).astype(jnp.bfloat16),
        'b_up': (0.3 * normal(weight_keys[9], (FF,))).astype(jnp.bfloat16),
        'w_down': (FF ** -0.5 * normal(weight_keys[10], (FF, D))).astype(jnp.bfloat16),
        'b_down': (0.3 * normal(weight_keys[11], (D,))).astype(jnp.bfloat16),
    }


def as_stored(values_in):
    return values_in + lax.stop_gradient(values_in.astype(jnp.bfloat16).astype(jnp.float32) - values_in)


def layer_norm(row_vals, norm_gain, norm_shift):
    row_mean = jnp.mean(row_vals, axis=-1, keepdims=True)
    centered = row_vals - row_mean
    row_var = jnp.mean(centered * centered, axis=-1, keepdims=True)
    return centered * lax.rsqrt(row_var + EPS) * norm_gain + norm_shift


def rope_tables():
    inv_freq = ROPE_BASE ** (-jnp.arange(0, ROT, 2, dtype=jnp.float32) / ROT)
    angles = jnp.arange(SEQ, dtype=jnp.float32)[:, None] * inv_freq[None, :]
    return jnp.cos(angles), jnp.sin(angles)


def rotary(head_vals, cos_t, sin_t):
    half_rot = ROT // 2
    first_half = head_vals[..., :half_rot]
    second_half = head_vals[..., half_rot:ROT]
    cos_b = cos_t[None, :, None, :]
    sin_b = sin_t[None, :, None, :]
    return jnp.concatenate([first_half * cos_b - second_half * sin_b, second_half * cos_b + first_half * sin_b, head_vals[..., ROT:]], axis=-1)


def causal_attention(q_all, k_all, v_all):
    n_blocks = SEQ // QBLK
    key_pos = jnp.arange(SEQ)

    def one_block(flat_idx):
        b_idx = flat_idx // n_blocks
        q_start = (flat_idx % n_blocks) * QBLK
        q_blk = lax.dynamic_slice(q_all, (b_idx, q_start, 0, 0), (1, QBLK, HEADS, HEAD))[0]
        k_row = lax.dynamic_index_in_dim(k_all, b_idx, axis=0, keepdims=False)
        v_row = lax.dynamic_index_in_dim(v_all, b_idx, axis=0, keepdims=False)
        scores = jnp.einsum('qhe,khe->hqk', q_blk, k_row) * HEAD ** -0.5
        q_pos = q_start + jnp.arange(QBLK)
        scores = jnp.where(key_pos[None, None, :] <= q_pos[None, :, None], scores, NEG_BIG)
        attn_probs = jax.nn.softmax(scores, axis=-1)
        return jnp.einsum('hqk,khe->qhe', attn_probs, v_row)

    block_outs = lax.map(jax.checkpoint(one_block), jnp.arange(BATCH * n_blocks))
    return block_outs.reshape(BATCH, SEQ, HEADS, HEAD)


def layer_forward(x_rows, ln1_gain, ln1_bias, ln2_gain, ln2_bias, w_qkv, b_qkv, w_out, b_out, w_up, b_up, w_down, b_down):
    cos_t, sin_t = rope_tables()
    h_attn = as_stored(layer_norm(x_rows, ln1_gain, ln1_bias))
    qkv_rows = jnp.einsum('bsd,dhce->bshce', h_attn, w_qkv) + b_qkv
    q_all = as_stored(rotary(qkv_rows[:, :, :, 0], cos_t, sin_t))
    k_all = as_stored(rotary(qkv_rows[:, :, :, 1], cos_t, sin_t))
    v_all = as_stored(qkv_rows[:, :, :, 2])
    attn_ctx = as_stored(causal_attention(q_all, k_all, v_all)).reshape(BATCH, SEQ, D)
    attn_proj = jnp.dot(attn_ctx, w_out) + b_out
    h_mlp = as_stored(layer_norm(x_rows, ln2_gain, ln2_bias))
    gelu_out = as_stored(jax.nn.gelu(jnp.dot(h_mlp, w_up) + b_up, approximate=False))
    mlp_proj = jnp.dot(gelu_out, w_down) + b_down
    return x_rows + attn_proj + mlp_proj


def reference(x_seq, dy_seq, ln1_gain, ln1_bias, ln2_gain, ln2_bias, w_qkv, b_qkv, w_out, b_out, w_up, b_up, w_down, b_down):
    y_full, back_fn = jax.vjp(layer_forward, x_seq.astype(jnp.float32), ln1_gain, ln1_bias, ln2_gain, ln2_bias, w_qkv.astype(jnp.float32), b_qkv.astype(jnp.float32), w_out.astype(jnp.float32), b_out.astype(jnp.float32), w_up.astype(jnp.float32), b_up.astype(jnp.float32), w_down.astype(jnp.float32), b_down.astype(jnp.float32))
    grads = back_fn(dy_seq)
    return (y_full.astype(jnp.bfloat16), grads[0], grads[1], grads[2], grads[3], grads[4], grads[5], grads[6], grads[7], grads[8], grads[9], grads[10], grads[11], grads[12])
```

```python
import functools
import math

import jax
import jax.numpy as jnp
from jax import lax
from jax.experimental import pallas as pl
from jax.experimental.pallas import tpu as pltpu
from jax.sharding import PartitionSpec as P

EPS = 1e-5
ROPE_BASE = 10000.0
NEG_BIG = -1e30
LOG2E = math.log2(math.e)
F32 = jnp.float32
BF16 = jnp.bfloat16


def dot(a, b):
    return jnp.dot(a, b, preferred_element_type=F32)


def dot_nt(a, b):
    return lax.dot_general(a, b, (((1,), (1,)), ((), ())), preferred_element_type=F32)


def layer_norm(row_vals, norm_gain, norm_shift):
    row_mean = jnp.mean(row_vals, axis=-1, keepdims=True)
    centered = row_vals - row_mean
    inv_std = lax.rsqrt(jnp.mean(centered * centered, axis=-1, keepdims=True) + EPS)
    x_norm = centered * inv_std
    return x_norm * norm_gain + norm_shift, x_norm, inv_std


def norm_backward(d_out, x_norm, inv_std, norm_gain):
    d_norm = d_out * norm_gain
    d_rows = inv_std * (d_norm - jnp.mean(d_norm, axis=-1, keepdims=True) - x_norm * jnp.mean(d_norm * x_norm, axis=-1, keepdims=True))
    return d_rows, jnp.sum(d_out * x_norm, axis=0), jnp.sum(d_out, axis=0)


def rope_tables(positions, head_dim):
    rot_dim = head_dim // 4
    inv_freq = ROPE_BASE ** (-2.0 * jnp.arange(rot_dim // 2, dtype=F32) / rot_dim)
    angles = inv_freq[:, None] * positions.astype(F32)[None, :]
    return jnp.cos(angles), jnp.sin(angles)


def rotate_t(head_vals, cos_t, sin_t):
    half = cos_t.shape[0]
    first = head_vals[:half]
    second = head_vals[half:2 * half]
    return jnp.concatenate([first * cos_t - second * sin_t, second * cos_t + first * sin_t, head_vals[2 * half:]], axis=0)


def pre_kernel(x_ref, gain_ref, bias_ref, w_ref, b_ref, cos_ref, sin_ref, h_ref, q_ref, k_ref, v_ref, kn_ref):
    head_dim = q_ref.shape[0]
    h_rows = layer_norm(x_ref[...].astype(F32), gain_ref[...], bias_ref[...])[0].astype(BF16)
    h_ref[...] = h_rows
    qkv = dot_nt(w_ref[...], h_rows) + b_ref[...]
    cos_t, sin_t = cos_ref[...], sin_ref[...]
    q_ref[...] = rotate_t(qkv[:head_dim], cos_t, sin_t).astype(BF16)
    k_t = rotate_t(qkv[head_dim:2 * head_dim], cos_t, sin_t)
    k_ref[...] = k_t.astype(BF16)
    kn_ref[...] = k_t.T.astype(BF16)
    v_ref[...] = qkv[2 * head_dim:].astype(BF16)


def pre_call(x_all, gain, bias, w_head, b_head, cos_t, sin_t, rows):
    seq, width = x_all.shape
    head_dim = w_head.shape[0] // 3
    half = cos_t.shape[0]
    whole = lambda shape: pl.BlockSpec(shape, lambda i: (0,) * len(shape))
    cols = lambda n: pl.BlockSpec((n, rows), lambda i: (0, i))
    return pl.pallas_call(
        pre_kernel,
        grid=(seq // rows,),
        in_specs=[pl.BlockSpec((rows, width), lambda i: (i, 0)), whole((1, width)), whole((1, width)),
                  whole(w_head.shape), whole(b_head.shape), cols(half), cols(half)],
        out_specs=[pl.BlockSpec((rows, width), lambda i: (i, 0)), cols(head_dim), cols(head_dim), cols(head_dim),
                   pl.BlockSpec((rows, head_dim), lambda i: (i, 0))],
        out_shape=[jax.ShapeDtypeStruct((seq, width), BF16)] + [jax.ShapeDtypeStruct((head_dim, seq), BF16)] * 3
        + [jax.ShapeDtypeStruct((seq, head_dim), BF16)],
        cost_estimate=pl.CostEstimate(flops=2 * seq * width * w_head.shape[0] * 3, bytes_accessed=seq * width * 4, transcendentals=0),
        name="pre",
    )(x_all, gain, bias, w_head, b_head, cos_t, sin_t)


def fwd_kernel(core_ref, kn_ref, q_ref, v_ref, ctx_ref, norm_ref, lse_ref, max_s, sum_s, acc_s, *, par, sub, scale2):
    step = pl.program_id(0)
    core = core_ref[0]
    rows = q_ref.shape[1]
    span = par * rows
    q_t = q_ref[...]

    def chunk(start, masked, first):
        score_list = []
        for j in range(span // sub):
            keys = kn_ref[pl.ds(pl.multiple_of(start + j * sub, sub), sub), :]
            scores = dot(keys, q_t)
            if masked:
                key_pos = j * sub + lax.broadcasted_iota(jnp.int32, scores.shape, 0)
                q_pos = core * rows + lax.broadcasted_iota(jnp.int32, scores.shape, 1)
                scores = jnp.where(key_pos <= q_pos, scores, NEG_BIG)
            score_list.append(scores)
        for j, scores in enumerate(score_list):
            blk_max = jnp.max(scores, axis=0, keepdims=True) * scale2
            fresh = first and j == 0
            old_max = None if fresh else max_s[...]
            new_max = blk_max if fresh else jnp.maximum(old_max, blk_max)
            probs = jnp.exp2(scores * scale2 - new_max)
            vals = v_ref[:, pl.ds(pl.multiple_of(start + j * sub, sub), sub)]
            part = dot(vals, probs.astype(BF16))
            part_sum = jnp.sum(probs, axis=0, keepdims=True)
            if fresh:
                sum_s[...] = part_sum
                acc_s[...] = part
            else:
                alpha = jnp.exp2(old_max - new_max)
                sum_s[...] = sum_s[...] * alpha + part_sum
                acc_s[...] = acc_s[...] * alpha + part
            max_s[...] = new_max

    chunk(step * span, True, True)

    @pl.loop(0, step)
    def _(i):
        chunk(i * span, False, False)

    total = sum_s[...]
    normed = acc_s[...] / total
    norm_ref[0] = normed
    ctx_ref[0] = normed.astype(BF16)
    lse_ref[0] = max_s[...] + jnp.log2(total)


def fwd_call(core, k_nat, q_t, v_t, rows, par, scale2):
    seq, head_dim = k_nat.shape
    steps = seq // (rows * par)
    sub = min(256, rows)
    pick = lambda i, core_ref: (0, i * par + core_ref[0])
    tile = lambda n: pl.BlockSpec((1, n, rows), lambda i, core_ref: (i, 0, 0))
    return pl.pallas_call(
        functools.partial(fwd_kernel, par=par, sub=sub, scale2=scale2),
        grid_spec=pltpu.PrefetchScalarGridSpec(
            num_scalar_prefetch=1, grid=(steps,),
            in_specs=[pl.BlockSpec((seq, head_dim), lambda i, core_ref: (0, 0)), pl.BlockSpec((head_dim, rows), pick),
                      pl.BlockSpec((head_dim, seq), lambda i, core_ref: (0, 0))],
            out_specs=[tile(head_dim), tile(head_dim), tile(1)],
            scratch_shapes=[pltpu.VMEM((1, rows), F32), pltpu.VMEM((1, rows), F32), pltpu.VMEM((head_dim, rows), F32)]),
        out_shape=[jax.ShapeDtypeStruct((steps, head_dim, rows), BF16), jax.ShapeDtypeStruct((steps, head_dim, rows), F32),
                   jax.ShapeDtypeStruct((steps, 1, rows), F32)],
        cost_estimate=pl.CostEstimate(flops=32 * seq * seq * head_dim // par, bytes_accessed=seq * head_dim * 8, transcendentals=seq * seq // 4),
        name="attn_fwd",
    )(core, k_nat, q_t, v_t)


def bwd_kernel(core_ref, k_ref, kn_ref, v_ref, q_ref, dy_ref, w_ref, ctx_ref, norm_ref, lse_ref,
               dq_ref, dk_ref, dv_ref, dw_ref, dq_s, *, par, sub, scale, scale2):
    step = pl.program_id(0)
    core = core_ref[0]
    rows = q_ref.shape[1]
    subs = rows // sub

    @pl.when(step == 0)
    def _():
        dk_ref[...] = jnp.zeros_like(dk_ref)
        dv_ref[...] = jnp.zeros_like(dv_ref)
        dw_ref[...] = jnp.zeros_like(dw_ref)

    q_t = q_ref[...]
    q_n = q_t.T
    dy_rows = dy_ref[0]
    d_ctx = dot_nt(w_ref[...], dy_rows)
    delta = jnp.sum(d_ctx * norm_ref[0], axis=0, keepdims=True)
    do_t = d_ctx.astype(BF16)
    do_n = do_t.T
    dw_ref[...] += dot(ctx_ref[0], dy_rows)
    lanes = 128
    spread = lambda row: jnp.concatenate([jnp.broadcast_to(row, (lanes, rows)).T] * (sub // lanes), axis=1)
    lse_c = spread(lse_ref[0])
    delta_c = spread(delta)
    dq_s[...] = jnp.zeros_like(dq_s)

    def chunk(i, masked):
        for b in range(par):
            for j in range(subs):
                cols = slice(j * sub, (j + 1) * sub)
                start = pl.multiple_of((i * par + b) * rows + j * sub, sub)
                k_t = k_ref[:, pl.ds(start, sub)]
                v_t = v_ref[:, pl.ds(start, sub)]
                probs = jnp.exp2(dot(q_n, k_t) * scale2 - lse_c)
                if masked:
                    key_pos = b * rows + j * sub + lax.broadcasted_iota(jnp.int32, probs.shape, 1)
                    q_pos = core * rows + lax.broadcasted_iota(jnp.int32, probs.shape, 0)
                    probs = jnp.where(key_pos <= q_pos, probs, 0.0)
                d_scores = (probs * (dot(do_n, v_t) - delta_c)).astype(BF16)
                dv_ref[i * par + b, :, cols] += dot(do_t, probs.astype(BF16))
                dk_ref[i * par + b, :, cols] += dot(q_t, d_scores)
                dq_s[...] += dot(d_scores, kn_ref[pl.ds(start, sub), :])

    chunk(step, True)

    @pl.loop(0, step)
    def _(i):
        chunk(i, False)

    dq_ref[0] = dq_s[...].T * scale


def bwd_call(core, k_t, k_nat, v_t, q_t, dy_all, w_head, ctx_t, norm_t, lse, rows, par, scale, scale2):
    seq, head_dim = k_nat.shape
    width = dy_all.shape[-1]
    steps = seq // (rows * par)
    sub = min(256, rows)
    whole = lambda shape: pl.BlockSpec(shape, lambda i, core_ref: (0,) * len(shape))
    tile = lambda n: pl.BlockSpec((1, n, rows), lambda i, core_ref: (i, 0, 0))
    return pl.pallas_call(
        functools.partial(bwd_kernel, par=par, sub=sub, scale=scale, scale2=scale2),
        grid_spec=pltpu.PrefetchScalarGridSpec(
            num_scalar_prefetch=1, grid=(steps,),
            in_specs=[whole((head_dim, seq)), whole((seq, head_dim)), whole((head_dim, seq)),
                      pl.BlockSpec((head_dim, rows), lambda i, core_ref: (0, i * par + core_ref[0])),
                      pl.BlockSpec((1, rows, width), lambda i, core_ref: (i * par + core_ref[0], 0, 0)),
                      whole((head_dim, width)), tile(head_dim), tile(head_dim), tile(1)],
            out_specs=[tile(head_dim), whole((steps * par, head_dim, rows)), whole((steps * par, head_dim, rows)), whole((head_dim, width))],
            scratch_shapes=[pltpu.VMEM((rows, head_dim), F32)]),
        out_shape=[jax.ShapeDtypeStruct((steps, head_dim, rows), F32), jax.ShapeDtypeStruct((steps * par, head_dim, rows), F32),
                   jax.ShapeDtypeStruct((steps * par, head_dim, rows), F32), jax.ShapeDtypeStruct((head_dim, width), F32)],
        cost_estimate=pl.CostEstimate(flops=64 * seq * seq * head_dim // par, bytes_accessed=seq * head_dim * 32, transcendentals=seq * seq // 4),
        name="attn_bwd",
    )(core, k_t, k_nat, v_t, q_t, dy_all.reshape(-1, rows, width), w_head, ctx_t, norm_t, lse)


def exact_gelu(pre_act):
    return jax.nn.gelu(pre_act, approximate=False)


def solution(mesh):
    cp_size = mesh.shape['cp']
    row_spec = P('dp', 'cp', None)
    in_specs = (row_spec, row_spec) + (P(),) * 12
    out_specs = (row_spec, row_spec, P('dp'), P('dp'), P('dp'), P('dp'), P('dp', None, None, None), P('dp', None, None), P('dp', None), P('dp'), P('dp', None), P('dp'), P('dp', None), P('dp'))

    def local_layer(x_blk, dy_blk, ln1_gain, ln1_bias, ln2_gain, ln2_bias, w_qkv, b_qkv, w_out, b_out, w_up, b_up, w_down, b_down):
        rows, width = x_blk.shape[1], x_blk.shape[2]
        heads, head_dim = w_qkv.shape[1], w_qkv.shape[3]
        par = cp_size // heads
        seq = rows * cp_size
        scale = head_dim ** -0.5
        scale2 = scale * LOG2E
        me = lax.axis_index('cp')
        head, core = me // par, me % par
        core_arr = jnp.reshape(core, (1,)).astype(jnp.int32)
        same_core = [[z * par + c for z in range(heads)] for c in range(par)]
        x_own, dy_own = x_blk[0], dy_blk[0]
        dy_bf = dy_own.astype(BF16)

        x_all = lax.all_gather(x_own, 'cp', tiled=True)
        dy_all = lax.all_gather(dy_bf, 'cp', tiled=True)

        x_rows = x_own.astype(F32)
        h_mlp, x_norm, inv_std = layer_norm(x_rows, ln2_gain, ln2_bias)
        h_mlp = h_mlp.astype(BF16)
        up_proj = dot(h_mlp, w_up) + b_up.astype(F32)
        gelu_out, gelu_back = jax.vjp(exact_gelu, up_proj)
        gelu_bf = gelu_out.astype(BF16)
        mlp_proj = dot(gelu_bf, w_down) + b_down.astype(F32)
        dy_sum = jnp.sum(dy_own, axis=0)
        d_w_down = dot(gelu_bf.T, dy_bf)
        d_up = gelu_back(dot_nt(dy_bf, w_down))[0]
        d_b_up = jnp.sum(d_up, axis=0)
        d_up_bf = d_up.astype(BF16)
        d_w_up = dot(h_mlp.T, d_up_bf)
        d_h_mlp = dot_nt(d_up_bf, w_up)
        dx_mlp, d_ln2_gain, d_ln2_bias = norm_backward(d_h_mlp, x_norm, inv_std, ln2_gain)
        early = lax.psum((d_w_up, d_w_down, d_b_up, dy_sum, d_ln2_gain, d_ln2_bias), 'cp')

        cos_t, sin_t = rope_tables(jnp.arange(seq), head_dim)
        w_head = lax.dynamic_index_in_dim(w_qkv, head, axis=1, keepdims=False).reshape(width, 3 * head_dim).T
        b_head = lax.dynamic_index_in_dim(b_qkv, head, axis=0, keepdims=False).reshape(3 * head_dim, 1).astype(F32)
        wo_head = lax.dynamic_slice_in_dim(w_out, head * head_dim, head_dim, axis=0)
        h_all, q_t, k_t, v_t, k_nat = pre_call(x_all, ln1_gain[None], ln1_bias[None], w_head, b_head, cos_t, sin_t, rows)
        ctx_t, norm_t, lse = fwd_call(core_arr, k_nat, q_t, v_t, rows, par, scale2)

        ctx_mine = lax.all_to_all(ctx_t, 'cp', 0, 0, axis_index_groups=same_core, tiled=True).reshape(width, rows)
        attn_proj = dot(ctx_mine.T, w_out) + b_out.astype(F32)
        y_rows = (x_rows + attn_proj + mlp_proj).astype(BF16)

        d_q, dk_part, dv_part, dwo_part = bwd_call(core_arr, k_t, k_nat, v_t, q_t, dy_all, wo_head, ctx_t, norm_t, lse, rows, par, scale, scale2)
        dkv_part = jnp.stack([dk_part, dv_part]).reshape(2, heads, par, head_dim, rows)
        other = lax.dynamic_index_in_dim(dkv_part, par - 1 - core, axis=2, keepdims=False)
        mine = lax.dynamic_index_in_dim(dkv_part, core, axis=2, keepdims=False)
        swap = [(z * par + c, z * par + par - 1 - c) for z in range(heads) for c in range(par)]
        d_k, d_v = mine + lax.ppermute(other, 'cp', swap)
        d_k = d_k * scale
        own_cos = lax.dynamic_index_in_dim(cos_t.reshape(-1, heads, par, rows), core, axis=2, keepdims=False)
        own_sin = lax.dynamic_index_in_dim(sin_t.reshape(-1, heads, par, rows), core, axis=2, keepdims=False)
        unrotate = jax.vmap(rotate_t, in_axes=(0, 1, 1))
        d_qkv = jnp.concatenate([unrotate(d_q, own_cos, -own_sin), unrotate(d_k, own_cos, -own_sin), d_v], axis=1)
        d_b_head = jnp.sum(d_qkv, axis=(0, 2))
        d_qkv = d_qkv.astype(BF16)
        d_qkv_mine = lax.all_to_all(d_qkv, 'cp', 0, 0, axis_index_groups=same_core, tiled=True).reshape(heads * 3 * head_dim, rows)
        d_h = lax.dot_general(d_qkv_mine, w_qkv.reshape(width, -1), (((0,), (1,)), ((), ())), preferred_element_type=F32)
        x_norm1 = x_norm
        dx_attn, d_ln1_gain, d_ln1_bias = norm_backward(d_h, x_norm1, inv_std, ln1_gain)
        dx_rows = dy_own + dx_attn + dx_mlp

        h_own = lax.dynamic_index_in_dim(h_all.reshape(heads, par, rows, width), core, axis=1, keepdims=False)
        d_w_head = jnp.einsum('ztd,zet->de', h_own, d_qkv, preferred_element_type=F32)
        d_w_full = jnp.zeros((width, heads, 3 * head_dim), F32)
        d_w_full = lax.dynamic_update_slice(d_w_full, d_w_head[:, None], (0, head, 0)).reshape(w_qkv.shape)
        d_b_full = lax.dynamic_update_slice(jnp.zeros((heads, 3 * head_dim), F32), d_b_head[None], (head, 0)).reshape(b_qkv.shape)
        d_wo_full = lax.dynamic_update_slice(jnp.zeros((width, width), F32), dwo_part, (head * head_dim, 0))
        late, early = lax.optimization_barrier(((d_w_full, d_b_full, d_wo_full, d_ln1_gain, d_ln1_bias), early))
        d_w_up, d_w_down, d_b_up, dy_sum, d_ln2_gain, d_ln2_bias = early
        d_w_qkv, d_b_qkv, d_w_out, d_ln1_gain, d_ln1_bias = lax.psum(late, 'cp')
        return (y_rows[None], dx_rows[None], d_ln1_gain, d_ln1_bias, d_ln2_gain, d_ln2_bias, d_w_qkv, d_b_qkv, d_w_out, dy_sum, d_w_up, d_b_up, d_w_down, dy_sum)

    return jax.shard_map(local_layer, mesh=mesh, in_specs=in_specs, out_specs=out_specs, check_vma=False)
```

```python
import functools
import math

import jax
import jax.numpy as jnp
from jax import lax
from jax.experimental import pallas as pl
from jax.experimental.pallas import tpu as pltpu
from jax.sharding import PartitionSpec as P


EPS = 1e-5
ROPE_BASE = 10000.0
NEG_BIG = -1e30
LOG2E = math.log2(math.e)
F32 = jnp.float32
BF16 = jnp.bfloat16


def dot(a, b):
    return jnp.dot(a, b, preferred_element_type=F32)


def dot_nt(a, b):
    return lax.dot_general(a, b, (((1,), (1,)), ((), ())), preferred_element_type=F32)


def layer_norm(row_vals, norm_gain, norm_shift):
    row_mean = jnp.mean(row_vals, axis=-1, keepdims=True)
    centered = row_vals - row_mean
    inv_std = lax.rsqrt(jnp.mean(centered * centered, axis=-1, keepdims=True) + EPS)
    x_norm = centered * inv_std
    return x_norm * norm_gain + norm_shift, x_norm, inv_std


def norm_backward(d_out, x_norm, inv_std, norm_gain):
    d_norm = d_out * norm_gain
    d_rows = inv_std * (d_norm - jnp.mean(d_norm, axis=-1, keepdims=True) - x_norm * jnp.mean(d_norm * x_norm, axis=-1, keepdims=True))
    return d_rows, jnp.sum(d_out * x_norm, axis=0), jnp.sum(d_out, axis=0)


def rope_tables(positions, head_dim):
    rot_dim = head_dim // 4
    inv_freq = ROPE_BASE ** (-2.0 * jnp.arange(rot_dim // 2, dtype=F32) / rot_dim)
    angles = inv_freq[:, None] * positions.astype(F32)[None, :]
    return jnp.cos(angles), jnp.sin(angles)


def rotate_t(head_vals, cos_t, sin_t):
    half = cos_t.shape[0]
    first = head_vals[:half]
    second = head_vals[half:2 * half]
    return jnp.concatenate([first * cos_t - second * sin_t, second * cos_t + first * sin_t, head_vals[2 * half:]], axis=0)


def pre_kernel(x_ref, gain_ref, bias_ref, gain2_ref, bias2_ref, w_ref, b_ref, cos_ref, sin_ref, h_ref, m_ref, q_ref, k_ref, v_ref, kn_ref):
    head_dim = q_ref.shape[0]
    x_norm = layer_norm(x_ref[...].astype(F32), 1.0, 0.0)[1]
    h_rows = (x_norm * gain_ref[...] + bias_ref[...]).astype(BF16)
    h_ref[...] = h_rows
    m_ref[...] = (x_norm * gain2_ref[...] + bias2_ref[...]).astype(BF16)
    qkv = dot_nt(w_ref[...], h_rows) + b_ref[...]
    cos_t, sin_t = cos_ref[...], sin_ref[...]
    q_ref[...] = rotate_t(qkv[:head_dim], cos_t, sin_t).astype(BF16)
    k_t = rotate_t(qkv[head_dim:2 * head_dim], cos_t, sin_t)
    k_ref[...] = k_t.astype(BF16)
    kn_ref[...] = k_t.T.astype(BF16)
    v_ref[...] = qkv[2 * head_dim:].astype(BF16)


def pre_call(x_all, gains, w_head, b_head, cos_t, sin_t, rows):
    seq, width = x_all.shape
    head_dim = w_head.shape[0] // 3
    half = cos_t.shape[0]
    whole = lambda shape: pl.BlockSpec(shape, lambda i: (0,) * len(shape))
    cols = lambda n: pl.BlockSpec((n, rows), lambda i: (0, i))
    wide = pl.BlockSpec((rows, width), lambda i: (i, 0))
    return pl.pallas_call(
        pre_kernel,
        grid=(seq // rows,),
        in_specs=[wide] + [whole((1, width))] * 4 + [whole(w_head.shape), whole(b_head.shape), cols(half), cols(half)],
        out_specs=[wide, wide, cols(head_dim), cols(head_dim), cols(head_dim), pl.BlockSpec((rows, head_dim), lambda i: (i, 0))],
        out_shape=[jax.ShapeDtypeStruct((seq, width), BF16)] * 2 + [jax.ShapeDtypeStruct((head_dim, seq), BF16)] * 3
        + [jax.ShapeDtypeStruct((seq, head_dim), BF16)],
        cost_estimate=pl.CostEstimate(flops=2 * seq * width * w_head.shape[0] * 3, bytes_accessed=seq * width * 6, transcendentals=0),
        name="pre",
    )(x_all, *gains, w_head, b_head, cos_t, sin_t)


def mlp_kernel(core_ref, m_ref, dy_ref, wu_ref, bu_ref, wd_ref, ctx_ref, dwu_ref, dwd_ref, dbu_ref, dwo_ref, *, par):
    step = pl.program_id(0)
    rows = ctx_ref.shape[2]

    @pl.when(step == 0)
    def _():
        for ref in (dwu_ref, dwd_ref, dbu_ref, dwo_ref):
            ref[...] = jnp.zeros_like(ref)

    m_rows, dy_rows = m_ref[...], dy_ref[...]
    up = dot_nt(wu_ref[...], m_rows) + bu_ref[...]
    cdf = 0.5 + 0.5 * lax.erf(up * (0.5 ** 0.5))
    gelu = (up * cdf).astype(BF16)
    d_gelu = dot_nt(wd_ref[...], dy_rows)
    d_up = d_gelu * (cdf + up * (jnp.exp(up * up * -0.5) * (2 * math.pi) ** -0.5))
    dwu_ref[...] += dot(d_up.astype(BF16), m_rows)
    dwd_ref[...] += dot(gelu, dy_rows)
    lanes = dbu_ref.shape[1]
    dbu_ref[...] += sum(d_up[:, i * lanes:(i + 1) * lanes] for i in range(d_up.shape[1] // lanes))
    own = pl.ds(pl.multiple_of(core_ref[0] * rows, rows), rows)
    dwo_ref[...] += dot(ctx_ref[0], dy_ref[own, :])


def mlp_call(core, m_all, dy_all, wu, bu, wd, ctx_t, par):
    seq, width = m_all.shape
    steps, head_dim, rows = ctx_t.shape
    span = seq // steps
    part = wu.shape[0]
    whole = lambda shape: pl.BlockSpec(shape, lambda i, core_ref: (0,) * len(shape))
    wide = pl.BlockSpec((span, width), lambda i, core_ref: (i, 0))
    return pl.pallas_call(
        functools.partial(mlp_kernel, par=par),
        grid_spec=pltpu.PrefetchScalarGridSpec(
            num_scalar_prefetch=1, grid=(steps,),
            in_specs=[wide, wide, whole((part, width)), whole((part, 1)), whole((part, width)),
                      pl.BlockSpec((1, head_dim, rows), lambda i, core_ref: (i, 0, 0))],
            out_specs=[whole((part, width)), whole((part, width)), whole((part, 128)), whole((head_dim, width))]),
        out_shape=[jax.ShapeDtypeStruct((part, width), F32), jax.ShapeDtypeStruct((part, width), F32),
                   jax.ShapeDtypeStruct((part, 128), F32), jax.ShapeDtypeStruct((head_dim, width), F32)],
        cost_estimate=pl.CostEstimate(flops=16 * seq * width * part, bytes_accessed=seq * width * 4, transcendentals=2 * seq * part),
        name="mlp_grad",
    )(core, m_all, dy_all, wu, bu, wd, ctx_t)


def fwd_kernel(core_ref, kn_ref, q_ref, v_ref, ctx_ref, norm_ref, lse_ref, max_s, sum_s, acc_s, *, par, sub, scale2):
    step = pl.program_id(0)
    core = core_ref[0]
    rows = q_ref.shape[1]
    span = par * rows
    q_t = q_ref[...]

    def chunk(start, masked, first):
        score_list = []
        for j in range(span // sub):
            keys = kn_ref[pl.ds(pl.multiple_of(start + j * sub, sub), sub), :]
            scores = dot(keys, q_t)
            if masked:
                key_pos = j * sub + lax.broadcasted_iota(jnp.int32, scores.shape, 0)
                q_pos = core * rows + lax.broadcasted_iota(jnp.int32, scores.shape, 1)
                scores = jnp.where(key_pos <= q_pos, scores, NEG_BIG)
            score_list.append(scores)
        for j, scores in enumerate(score_list):
            blk_max = jnp.max(scores, axis=0, keepdims=True) * scale2
            fresh = first and j == 0
            old_max = None if fresh else max_s[...]
            new_max = blk_max if fresh else jnp.maximum(old_max, blk_max)
            probs = jnp.exp2(scores * scale2 - new_max)
            vals = v_ref[:, pl.ds(pl.multiple_of(start + j * sub, sub), sub)]
            part = dot(vals, probs.astype(BF16))
            part_sum = jnp.sum(probs, axis=0, keepdims=True)
            if fresh:
                sum_s[...] = part_sum
                acc_s[...] = part
            else:
                alpha = jnp.exp2(old_max - new_max)
                sum_s[...] = sum_s[...] * alpha + part_sum
                acc_s[...] = acc_s[...] * alpha + part
            max_s[...] = new_max

    chunk(step * span, True, True)

    @pl.loop(0, step)
    def _(i):
        chunk(i * span, False, False)

    total = sum_s[...]
    normed = acc_s[...] / total
    norm_ref[0] = normed
    ctx_ref[0] = normed.astype(BF16)
    lse_ref[0] = max_s[...] + jnp.log2(total)


def fwd_call(core, k_nat, q_t, v_t, rows, par, scale2):
    seq, head_dim = k_nat.shape
    steps = seq // (rows * par)
    sub = min(256, rows)
    pick = lambda i, core_ref: (0, i * par + core_ref[0])
    tile = lambda n: pl.BlockSpec((1, n, rows), lambda i, core_ref: (i, 0, 0))
    return pl.pallas_call(
        functools.partial(fwd_kernel, par=par, sub=sub, scale2=scale2),
        grid_spec=pltpu.PrefetchScalarGridSpec(
            num_scalar_prefetch=1, grid=(steps,),
            in_specs=[pl.BlockSpec((seq, head_dim), lambda i, core_ref: (0, 0)), pl.BlockSpec((head_dim, rows), pick),
                      pl.BlockSpec((head_dim, seq), lambda i, core_ref: (0, 0))],
            out_specs=[tile(head_dim), tile(head_dim), tile(1)],
            scratch_shapes=[pltpu.VMEM((1, rows), F32), pltpu.VMEM((1, rows), F32), pltpu.VMEM((head_dim, rows), F32)]),
        out_shape=[jax.ShapeDtypeStruct((steps, head_dim, rows), BF16), jax.ShapeDtypeStruct((steps, head_dim, rows), F32),
                   jax.ShapeDtypeStruct((steps, 1, rows), F32)],
        cost_estimate=pl.CostEstimate(flops=32 * seq * seq * head_dim // par, bytes_accessed=seq * head_dim * 8, transcendentals=seq * seq // 4),
        name="attn_fwd",
    )(core, k_nat, q_t, v_t)


def bwd_kernel(core_ref, k_ref, kn_ref, v_ref, q_ref, dy_ref, w_ref, norm_ref, lse_ref,
               dq_ref, dkv_ref, dq_s, *, par, sub, scale, scale2):
    step = pl.program_id(0)
    core = core_ref[0]
    rows = q_ref.shape[1]
    subs = rows // sub

    @pl.when(step == 0)
    def _():
        dkv_ref[...] = jnp.zeros_like(dkv_ref)

    q_t = q_ref[...]
    q_n = q_t.T
    dy_rows = dy_ref[0]
    d_ctx = dot_nt(w_ref[...], dy_rows)
    delta = jnp.sum(d_ctx * norm_ref[0], axis=0, keepdims=True)
    do_t = d_ctx.astype(BF16)
    do_n = do_t.T
    lanes = 128
    spread = lambda row: jnp.concatenate([jnp.broadcast_to(row, (lanes, rows)).T] * (sub // lanes), axis=1)
    lse_c = spread(lse_ref[0])
    delta_c = spread(delta)
    dq_s[...] = jnp.zeros_like(dq_s)

    def chunk(i, masked):
        for b in range(par):
            for j in range(subs):
                cols = slice(j * sub, (j + 1) * sub)
                start = pl.multiple_of((i * par + b) * rows + j * sub, sub)
                k_t = k_ref[:, pl.ds(start, sub)]
                v_t = v_ref[:, pl.ds(start, sub)]
                probs = jnp.exp2(dot(q_n, k_t) * scale2 - lse_c)
                if masked:
                    key_pos = b * rows + j * sub + lax.broadcasted_iota(jnp.int32, probs.shape, 1)
                    q_pos = core * rows + lax.broadcasted_iota(jnp.int32, probs.shape, 0)
                    probs = jnp.where(key_pos <= q_pos, probs, 0.0)
                d_scores = (probs * (dot(do_n, v_t) - delta_c)).astype(BF16)
                rel = lax.rem(core + b, par)
                dkv_ref[rel, 1, i, :, cols] += dot(do_t, probs.astype(BF16))
                dkv_ref[rel, 0, i, :, cols] += dot(q_t, d_scores)
                dq_s[...] += dot(d_scores, kn_ref[pl.ds(start, sub), :])

    chunk(step, True)

    @pl.loop(0, step)
    def _(i):
        chunk(i, False)

    dq_ref[0] = dq_s[...].T * scale


def bwd_call(core, k_t, k_nat, v_t, q_t, dy_all, w_head, norm_t, lse, rows, par, scale, scale2):
    seq, head_dim = k_nat.shape
    width = dy_all.shape[-1]
    steps = seq // (rows * par)
    sub = min(256, rows)
    whole = lambda shape: pl.BlockSpec(shape, lambda i, core_ref: (0,) * len(shape))
    tile = lambda n: pl.BlockSpec((1, n, rows), lambda i, core_ref: (i, 0, 0))
    return pl.pallas_call(
        functools.partial(bwd_kernel, par=par, sub=sub, scale=scale, scale2=scale2),
        grid_spec=pltpu.PrefetchScalarGridSpec(
            num_scalar_prefetch=1, grid=(steps,),
            in_specs=[whole((head_dim, seq)), whole((seq, head_dim)), whole((head_dim, seq)),
                      pl.BlockSpec((head_dim, rows), lambda i, core_ref: (0, i * par + core_ref[0])),
                      pl.BlockSpec((1, rows, width), lambda i, core_ref: (i * par + core_ref[0], 0, 0)),
                      whole((head_dim, width)), tile(head_dim), tile(1)],
            out_specs=[tile(head_dim), whole((par, 2, steps, head_dim, rows))],
            scratch_shapes=[pltpu.VMEM((rows, head_dim), F32)]),
        out_shape=[jax.ShapeDtypeStruct((steps, head_dim, rows), F32), jax.ShapeDtypeStruct((par, 2, steps, head_dim, rows), F32)],
        cost_estimate=pl.CostEstimate(flops=64 * seq * seq * head_dim // par, bytes_accessed=seq * head_dim * 32, transcendentals=seq * seq // 4),
        name="attn_bwd",
    )(core, k_t, k_nat, v_t, q_t, dy_all.reshape(-1, rows, width), w_head, norm_t, lse)


def post_kernel(core_ref, dq_ref, mine_ref, got_ref, cos_ref, sin_ref, h_ref, out_ref, dw_ref, db_ref, *, scale):
    @pl.when(pl.program_id(0) == 0)
    def _():
        dw_ref[...] = jnp.zeros_like(dw_ref)
        db_ref[...] = jnp.zeros_like(db_ref)

    cos_t, sin_t = cos_ref[...], -sin_ref[...]
    d_q = rotate_t(dq_ref[0], cos_t, sin_t)
    d_k = rotate_t((mine_ref[0, 0, 0] + got_ref[0, 0]) * scale, cos_t, sin_t)
    d_v = mine_ref[0, 1, 0] + got_ref[1, 0]
    d_qkv = jnp.concatenate([d_q, d_k, d_v], axis=0)
    lanes = db_ref.shape[1]
    db_ref[...] += sum(d_qkv[:, i * lanes:(i + 1) * lanes] for i in range(d_qkv.shape[1] // lanes))
    d_qkv = d_qkv.astype(BF16)
    out_ref[0] = d_qkv
    dw_ref[...] += dot(d_qkv, h_ref[...])


def post_call(core, d_q, dkv, got, cos_t, sin_t, h_all, par, scale):
    steps, head_dim, rows = d_q.shape
    width = h_all.shape[1]
    half = cos_t.shape[0]
    own_cols = pl.BlockSpec((half, rows), lambda i, core_ref: (0, i * par + core_ref[0]))
    whole = lambda shape: pl.BlockSpec(shape, lambda i, core_ref: (0,) * len(shape))
    return pl.pallas_call(
        functools.partial(post_kernel, scale=scale),
        grid_spec=pltpu.PrefetchScalarGridSpec(
            num_scalar_prefetch=1, grid=(steps,),
            in_specs=[pl.BlockSpec((1, head_dim, rows), lambda i, core_ref: (i, 0, 0)),
                      pl.BlockSpec((1, 2, 1, head_dim, rows), lambda i, core_ref: (0, 0, i, 0, 0)),
                      pl.BlockSpec((2, 1, head_dim, rows), lambda i, core_ref: (0, i, 0, 0)),
                      own_cols, own_cols, pl.BlockSpec((rows, width), lambda i, core_ref: (i * par + core_ref[0], 0))],
            out_specs=[pl.BlockSpec((1, 3 * head_dim, rows), lambda i, core_ref: (i, 0, 0)), whole((3 * head_dim, width)), whole((3 * head_dim, 128))]),
        out_shape=[jax.ShapeDtypeStruct((steps, 3 * head_dim, rows), BF16), jax.ShapeDtypeStruct((3 * head_dim, width), F32),
                   jax.ShapeDtypeStruct((3 * head_dim, 128), F32)],
        cost_estimate=pl.CostEstimate(flops=6 * steps * head_dim * rows * width, bytes_accessed=steps * rows * width * 4, transcendentals=0),
        name="post",
    )(core, d_q, dkv, got, cos_t, sin_t, h_all)


def share_kernel(x_ref, o_ref, held, send_sem, recv_sem, *, size):
    me = lax.axis_index('cp')
    barrier = pltpu.get_barrier_semaphore()
    for i in range(1, size):
        pl.semaphore_signal(barrier, inc=1, device_id={'cp': lax.rem(me + i, size)}, device_id_type=pl.DeviceIdType.MESH)
    pl.semaphore_wait(barrier, size - 1)
    copies = []
    for i in range(1, size):
        copy = pltpu.make_async_remote_copy(src_ref=x_ref, dst_ref=held.at[i - 1], send_sem=send_sem.at[i - 1], recv_sem=recv_sem.at[i - 1],
                                            device_id={'cp': lax.rem(me + i, size)}, device_id_type=pl.DeviceIdType.MESH)
        copy.start()
        copies.append(copy)
    o_ref[0] = x_ref[...]
    for i in range(1, size):
        copies[i - 1].wait()
        o_ref[i] = held[i - 1]


def share_call(vec, size):
    rows, lanes = vec.shape
    spec = pl.BlockSpec(memory_space=pltpu.VMEM)
    return pl.pallas_call(
        functools.partial(share_kernel, size=size),
        in_specs=[spec], out_specs=spec,
        out_shape=jax.ShapeDtypeStruct((size, rows, lanes), F32),
        scratch_shapes=[pltpu.VMEM((size - 1, rows, lanes), F32), pltpu.SemaphoreType.DMA((size - 1,)), pltpu.SemaphoreType.DMA((size - 1,))],
        compiler_params=pltpu.CompilerParams(collective_id=0, has_side_effects=True),
        name="share",
    )(vec)


def exact_gelu(pre_act):
    return jax.nn.gelu(pre_act, approximate=False)


def solution(mesh):
    cp_size = mesh.shape['cp']
    row_spec = P('dp', 'cp', None)
    in_specs = (row_spec, row_spec) + (P(),) * 12
    out_specs = (row_spec, row_spec, P('dp'), P('dp'), P('dp'), P('dp'), P('dp', None, None, None), P('dp', None, None), P('dp', None), P('dp'), P('dp', None), P('dp'), P('dp', None), P('dp'))

    def local_layer(x_blk, dy_blk, ln1_gain, ln1_bias, ln2_gain, ln2_bias, w_qkv, b_qkv, w_out, b_out, w_up, b_up, w_down, b_down):
        rows, width = x_blk.shape[1], x_blk.shape[2]
        heads, head_dim = w_qkv.shape[1], w_qkv.shape[3]
        par = cp_size // heads
        seq = rows * cp_size
        scale = head_dim ** -0.5
        scale2 = scale * LOG2E
        me = lax.axis_index('cp')
        head, core = me // par, me % par
        core_arr = jnp.reshape(core, (1,)).astype(jnp.int32)
        same_core = [[z * par + c for z in range(heads)] for c in range(par)]
        x_own, dy_own = x_blk[0], dy_blk[0]
        dy_bf = dy_own.astype(BF16)

        x_all = lax.all_gather(x_own, 'cp', tiled=True)
        dy_all = lax.all_gather(dy_bf, 'cp', tiled=True)

        x_rows = x_own.astype(F32)
        h_mlp, x_norm, inv_std = layer_norm(x_rows, ln2_gain, ln2_bias)
        h_mlp = h_mlp.astype(BF16)
        up_proj = dot(h_mlp, w_up) + b_up.astype(F32)
        gelu_out, gelu_back = jax.vjp(exact_gelu, up_proj)
        mlp_proj = dot(gelu_out.astype(BF16), w_down) + b_down.astype(F32)
        dy_sum = jnp.sum(dy_own, axis=0)
        d_up = gelu_back(dot_nt(dy_bf, w_down))[0]
        d_h_mlp = dot_nt(d_up.astype(BF16), w_up)
        dx_mlp, d_ln2_gain, d_ln2_bias = norm_backward(d_h_mlp, x_norm, inv_std, ln2_gain)
        y_part = x_rows + mlp_proj + b_out.astype(F32)
        dx_part = dy_own + dx_mlp

        ff = w_up.shape[1]
        part = ff // cp_size
        cos_t, sin_t = rope_tables(jnp.arange(seq), head_dim)
        w_head = lax.dynamic_index_in_dim(w_qkv, head, axis=1, keepdims=False).reshape(width, 3 * head_dim).T
        b_head = lax.dynamic_index_in_dim(b_qkv, head, axis=0, keepdims=False).reshape(3 * head_dim, 1).astype(F32)
        wo_head = lax.dynamic_slice_in_dim(w_out, head * head_dim, head_dim, axis=0)
        wu_part = lax.dynamic_slice_in_dim(w_up, me * part, part, axis=1).T
        bu_part = lax.dynamic_slice_in_dim(b_up, me * part, part, axis=0).astype(F32)[:, None]
        wd_part = lax.dynamic_slice_in_dim(w_down, me * part, part, axis=0)
        gains = (ln1_gain[None], ln1_bias[None], ln2_gain[None], ln2_bias[None])
        x_all, y_part, dx_part = lax.optimization_barrier((x_all, y_part, dx_part))
        h_all, m_all, q_t, k_t, v_t, k_nat = pre_call(x_all, gains, w_head, b_head, cos_t, sin_t, rows * par)
        ctx_t, norm_t, lse = fwd_call(core_arr, k_nat, q_t, v_t, rows, par, scale2)
        ctx_parts, w_parts = [], []
        w_heads = w_out.reshape(heads, head_dim, width)
        for d in range(heads):
            piece = lax.dynamic_index_in_dim(ctx_t, lax.rem(head + d, heads), keepdims=False)
            away = [(z * par + c, (z + d) % heads * par + c) for z in range(heads) for c in range(par)]
            ctx_parts.append(piece if d == 0 else lax.ppermute(piece, 'cp', away))
            w_parts.append(lax.dynamic_index_in_dim(w_heads, lax.rem(head - d + heads, heads), keepdims=False))
        d_wu, d_wd, d_bu, d_wo = mlp_call(core_arr, m_all, dy_all, wu_part, bu_part, wd_part, ctx_t, par)
        d_w_up_t = lax.all_gather(d_wu, 'cp', tiled=True)
        d_w_down = lax.all_gather(d_wd, 'cp', tiled=True)
        d_w_out = lax.all_gather(d_wo, 'cp')
        lse, d_wu = lax.optimization_barrier((lse, d_wu))
        d_q, dkv = bwd_call(core_arr, k_t, k_nat, v_t, q_t, dy_all, wo_head, norm_t, lse, rows, par, scale, scale2)
        d_w_up = d_w_up_t.T
        d_w_out = jnp.sum(d_w_out.reshape(heads, par, head_dim, width), axis=1).reshape(width, width)
        ctx_mine, w_mine = jnp.concatenate(ctx_parts, axis=0), jnp.concatenate(w_parts, axis=0)
        attn_proj = lax.dot_general(ctx_mine, w_mine, (((0,), (0,)), ((), ())), preferred_element_type=F32)
        y_rows = (y_part + attn_proj).astype(BF16)

        swap = [(z * par + c, z * par + par - 1 - c) for z in range(heads) for c in range(par)]
        got = lax.ppermute(dkv[1], 'cp', swap)
        d_qkv, d_w_head, d_b_head = post_call(core_arr, d_q, dkv, got, cos_t, sin_t, h_all, par, scale)
        d_qkv_mine = lax.all_to_all(d_qkv, 'cp', 0, 0, axis_index_groups=same_core, tiled=True).reshape(heads * 3 * head_dim, rows)
        halves = d_w_head.reshape(par, -1, width)
        d_w_half = lax.dynamic_index_in_dim(halves, core, keepdims=False) + lax.ppermute(lax.dynamic_index_in_dim(halves, par - 1 - core, keepdims=False), 'cp', swap)
        d_w_qkv_t = lax.all_gather(d_w_half, 'cp', tiled=True)
        d_w_qkv = d_w_qkv_t.T.reshape(w_qkv.shape)
        d_h = lax.dot_general(d_qkv_mine, w_qkv.reshape(width, -1), (((0,), (1,)), ((), ())), preferred_element_type=F32)
        dx_attn, d_ln1_gain, d_ln1_bias = norm_backward(d_h, x_norm, inv_std, ln1_gain)
        dx_rows = dx_part + dx_attn

        small = [d_ln1_gain, d_ln1_bias, d_ln2_gain, d_ln2_bias, dy_sum, jnp.sum(d_b_head, axis=1), jnp.sum(d_bu, axis=1)]
        sizes = [v.shape[0] for v in small]
        total = sum(sizes)
        padded = -(-total // 1024) * 1024
        vec = jnp.concatenate(small + [jnp.zeros((padded - total,), F32)]).reshape(-1, 128)
        shared = share_call(vec, cp_size).reshape(cp_size, padded)
        ends = [sum(sizes[:i]) for i in range(len(sizes) + 1)]
        sums = jnp.sum(shared[:, :ends[5]], axis=0)
        d_ln1_gain, d_ln1_bias, d_ln2_gain, d_ln2_bias, dy_sum = (sums[ends[i]:ends[i + 1]] for i in range(5))
        origin = lax.rem(me - jnp.arange(cp_size) + cp_size, cp_size)
        place = (origin[None, :] == jnp.arange(cp_size)[:, None])[:, :, None]
        ordered = jnp.sum(jnp.where(place, shared[None, :, ends[5]:ends[7]], 0.0), axis=1)
        d_b_qkv = jnp.sum(ordered[:, :sizes[5]].reshape(heads, par, -1), axis=1).reshape(b_qkv.shape)
        d_b_up = ordered[:, sizes[5]:].reshape(ff)
        return (y_rows[None], dx_rows[None], d_ln1_gain, d_ln1_bias, d_ln2_gain, d_ln2_bias, d_w_qkv, d_b_qkv, d_w_out, dy_sum, d_w_up, d_b_up, d_w_down, dy_sum)

    return jax.shard_map(local_layer, mesh=mesh, in_specs=in_specs, out_specs=out_specs, check_vma=False)
```
